32 devices in a mesh: kx: 2 (over x), ky: 4 (over y, core), kz: 4 (over z).
Axes of the slice: x: 2, y: 2, z: 4, core: 2. Of those that a mesh axis runs over, the one named last changes fastest.
Arguments:
- coefficients: bfloat16 [2, 2, 4, 4, 512, 2048], P(None, 'kx', 'ky', 'kz'), may hold values from -1 to 1
- shift_blocks: int32 [3], replicated, may hold values from 1 to 15, as said below
Outputs:
- centre: float32 [3, 512], replicated
- spread: float32 [3, 512], replicated
- coherence: float32 [3, 2, 4, 4], P(None, 'kx', 'ky', 'kz')
The draws below stay inside these ranges and needn't reach their ends.
Inputs may be any that keep to these rules, and one draw needn't show every extreme that they name: The coefficients one period further along direction d are those of the first k-point of the string with plane-wave index g read at (g + 128 * shift_blocks[d]) mod 2048.
All inputs are finite; a program needn't handle non-finite values.
Results may differ from the reference program's by a relative error of at most 0.0003.
Values may be sent and summed in bfloat16 or wider, within the bound.
A program may use at most 128 MiB of HBM per device.

```python
import jax
import jax.numpy as jnp
from jax import lax

NB = 512
NGW = 2048
NX = 2
NY = 4
NZ = 4


def offsets_for(key):
    middle = jax.random.randint(jax.random.fold_in(key, 11), (1,), 1, NGW // 128).astype(jnp.int32)
    ends = jnp.array([1, NGW // 128 - 1], jnp.int32)
    values = jnp.concatenate([ends, middle])
    order = jax.random.permutation(jax.random.fold_in(key, 13), 3)
    return values[order].astype(jnp.int32)


def draw_shift_blocks(key, part):
    return offsets_for(key)


def mix_along(fields, shift, points, position):
    angles = jnp.arange(points, dtype=jnp.float32) * (jnp.pi / (2.0 * points))
    dims_shape = [1] * (fields.ndim + 1)
    dims_shape[position] = points
    cosine = jnp.cos(angles).reshape(dims_shape)
    sine = jnp.sin(angles).reshape(dims_shape)
    rolled = jnp.roll(fields, -shift, axis=-1)
    return cosine * jnp.expand_dims(fields, position) + sine * jnp.expand_dims(rolled, position)


def draw_coefficients(key, part):
    offsets = offsets_for(key) * 128
    subkeys = jax.random.split(jax.random.fold_in(key, 23), 5)
    entry_scale = 1.0 / jnp.sqrt(2.0 * NGW)
    common = jnp.clip(jax.random.normal(subkeys[0], (2, NB, NGW), jnp.float32), -6.0, 6.0) * entry_scale
    fields = mix_along(common, offsets[2], NZ, 1)
    fields = mix_along(fields, offsets[1], NY, 1)
    fields = mix_along(fields, offsets[0], NX, 1)
    full_shape = (2, NX, NY, NZ, NB, NGW)
    roughness = jnp.clip(jax.random.normal(subkeys[1], full_shape, jnp.float32), -6.0, 6.0)
    amplitude = jnp.exp(jax.random.uniform(subkeys[2], (NB,), jnp.float32, jnp.log(0.1), jnp.log(0.6)))
    jitter = 0.35
    fields = fields + amplitude[:, None] * roughness * entry_scale
    winding = jax.random.uniform(subkeys[3], (3, NB), jnp.float32, -0.2, 0.2)
    x_frac = jnp.arange(NX, dtype=jnp.float32) / NX
    y_frac = jnp.arange(NY, dtype=jnp.float32) / NY
    z_frac = jnp.arange(NZ, dtype=jnp.float32) / NZ
    angles = 2.0 * jnp.pi * (winding[0] * x_frac[:, None, None, None] + winding[1] * y_frac[None, :, None, None] + winding[2] * z_frac[None, None, :, None])
    angles = angles + jax.random.uniform(subkeys[4], (NX, NY, NZ, NB), jnp.float32, -jitter, jitter)
    cosine = jnp.cos(angles)[..., None]
    sine = jnp.sin(angles)[..., None]
    real_part = cosine * fields[0] - sine * fields[1]
    imag_part = sine * fields[0] + cosine * fields[1]
    return jnp.stack([real_part, imag_part]).astype(jnp.bfloat16)


def setup_inputs(seed: int = 0) -> dict:
    arg_keys = jax.random.split(jax.random.key(seed), 3)
    coefficients = draw_coefficients(jax.random.fold_in(arg_keys[2], 71), 0)
    shift_blocks = draw_shift_blocks(jax.random.fold_in(arg_keys[2], 71), 0)
    return dict(coefficients=coefficients, shift_blocks=shift_blocks)


def pair_measure(own_point, partner):
    bands = own_point.shape[1]
    left_side = jnp.concatenate([own_point[0], own_point[1]], axis=1)
    right_side = jnp.concatenate([jnp.concatenate([partner[0], partner[1]], axis=1), jnp.concatenate([partner[1], -partner[0]], axis=1)], axis=0)
    product = jnp.dot(left_side, right_side.T, preferred_element_type=jnp.float32)
    real_part = product[:, :bands]
    imag_part = product[:, bands:]
    phases = jnp.arctan2(jnp.diagonal(imag_part), jnp.diagonal(real_part))
    coherence = jnp.sum(real_part * real_part + imag_part * imag_part) / bands
    return phases, coherence


def reference(coefficients, shift_blocks):
    shifts = shift_blocks.astype(jnp.int32) * 128
    k_total = NX * NY * NZ
    counts = jnp.array([NX, NY, NZ], jnp.float32)

    def per_point(k_index):
        x_index = k_index // (NY * NZ)
        y_index = (k_index // NZ) % NY
        z_index = k_index % NZ
        own_point = coefficients[:, x_index, y_index, z_index]
        gathered_phases = []
        gathered_coherence = []
        for direction in range(3):
            coords = [x_index, y_index, z_index]
            limits = [NX, NY, NZ]
            wrapped = coords[direction] == limits[direction] - 1
            coords[direction] = (coords[direction] + 1) % limits[direction]
            partner = coefficients[:, coords[0], coords[1], coords[2]]
            partner = jnp.where(wrapped, jnp.roll(partner, -shifts[direction], axis=-1), partner)
            phases, coherence = pair_measure(own_point, partner)
            gathered_phases.append(phases)
            gathered_coherence.append(coherence)
        return jnp.stack(gathered_phases), jnp.stack(gathered_coherence)

    phases, coherence = lax.map(per_point, jnp.arange(k_total, dtype=jnp.int32))
    mean_phase = jnp.sum(phases, axis=0) / k_total
    deviation = phases - mean_phase[None]
    variance = jnp.sum(deviation * deviation, axis=0) / k_total
    centre = -counts[:, None] * mean_phase / (2.0 * jnp.pi)
    spread = (counts[:, None] / (2.0 * jnp.pi)) ** 2 * variance
    coherence_out = coherence.T.reshape(3, NX, NY, NZ)
    return centre, spread, coherence_out
```

```python
import functools

import jax
import jax.numpy as jnp
from jax import lax
from jax.experimental import pallas as pl
from jax.experimental.pallas import tpu as pltpu
from jax.sharding import PartitionSpec as P

MESH = pl.DeviceIdType.MESH
AXES = ("kx", "ky", "kz")
LANES = 128
ROWS = 256
STRIP = 32


def greeted(count):
    return range(1, count) if count > 4 else sorted({1, count - 1})


def merged(parts, count):
    mean = functools.reduce(jnp.add, [part[0] for part in parts]) / len(parts)
    square = functools.reduce(jnp.add, [part[1] for part in parts])
    apart = functools.reduce(jnp.add, [(part[0] - mean) * (part[0] - mean) for part in parts])
    return mean, square + count * apart


def kernel(sizes, shift_ref, a_ref, centre_ref, spread_ref, coherence_ref,
           own, partner, rolled, diag_re, diag_im, total, stats, heard,
           own_sem, send_sem, recv_sem, stat_send, stat_recv):
    planes, bands, width = own.shape[1:]
    chunks, cut = partner.shape[1], partner.shape[3]
    tiles, row_tiles = width // LANES, bands // ROWS
    place = [lax.axis_index(axis) for axis in AXES]
    points = [(d, p) for d in range(3) for p in range(planes)]

    def beside(d, step):
        return {AXES[d]: lax.rem(place[d] + step, sizes[d])}

    load = pltpu.make_async_copy(a_ref, own, own_sem)
    load.start()
    barrier = pltpu.get_barrier_semaphore()
    greetings = 0
    for d in range(3):
        for step in greeted(sizes[d]):
            pl.semaphore_signal(barrier, inc=1, device_id=beside(d, step), device_id_type=MESH)
            greetings += 1
    pl.semaphore_wait(barrier, greetings)

    def copy_of(i, c):
        d, p = points[i]
        source = (p + 1) % planes if d == 0 else p
        return pltpu.make_async_remote_copy(
            src_ref=a_ref.at[:, source, pl.ds(pl.multiple_of(c * cut, cut), cut), :],
            dst_ref=partner.at[i, c],
            send_sem=send_sem.at[i, c],
            recv_sem=recv_sem.at[i, c],
            device_id=beside(d, sizes[d] - 1),
            device_id_type=MESH,
        )

    def inner_copy(i, c):
        p = points[i][1]
        return pltpu.make_async_copy(
            a_ref.at[:, p + 1, pl.ds(pl.multiple_of(c * cut, cut), cut), :], partner.at[i, c], recv_sem.at[i, c]
        )

    def inner(i):
        d, p = points[i]
        return d == 0 and p < planes - 1

    def launch(c, carry):
        for i in range(len(points)):
            (inner_copy(i, c) if inner(i) else copy_of(i, c)).start()
        return carry

    lax.fori_loop(0, chunks, launch, 0)

    total[...] = jnp.zeros_like(total)
    diag_re[...] = jnp.zeros_like(diag_re)
    diag_im[...] = jnp.zeros_like(diag_im)
    load.wait()
    for i, (d, p) in enumerate(points):
        wraps = place[d] == sizes[d] - 1
        shift = 0 if inner(i) else jnp.where(wraps, shift_ref[d], 0)

        moves = [] if inner(i) else [(LANES << bit, (shift >> bit) & 1 == 1) for bit in range((tiles - 1).bit_length())]

        def turn(block, carry, i=i, p=p, moves=moves):
            rows = pl.ds(pl.multiple_of(block * STRIP, STRIP), STRIP)
            for part in range(2):
                value = own[part, p, rows, :]
                for amount, taken in moves:
                    moved = jnp.concatenate([value[:, width - amount:], value[:, :width - amount]], axis=1)
                    value = jnp.where(taken, moved, value)
                rolled[i, part, rows, :] = value
            return carry

        lax.fori_loop(0, bands // STRIP, turn, 0)

    row = lax.broadcasted_iota(jnp.int32, (ROWS, cut), 0)
    column = lax.broadcasted_iota(jnp.int32, (ROWS, cut), 1)

    def arrived(i, c):
        (inner_copy(i, c).wait if inner(i) else copy_of(i, c).wait_recv)()

    def measure(i, c, r):
        left = rolled[i, :, pl.ds(pl.multiple_of(r * ROWS, ROWS), ROWS), :].reshape(2 * ROWS, width)
        right = partner[i, c].reshape(2 * cut, width)
        product = lax.dot_general(left, right, (((1,), (1,)), ((), ())), preferred_element_type=jnp.float32)
        re = product[:ROWS, :cut] + product[ROWS:, cut:]
        im = product[:ROWS, cut:] - product[ROWS:, :cut]
        squares = re * re + im * im
        total[i] += jnp.sum(squares.reshape(ROWS // 8, 8, cut), axis=0)
        same = row + r * ROWS == column + c * cut
        diag_re[i, pl.ds(c, 1), :] += jnp.sum(jnp.where(same, re, 0.0), axis=0, keepdims=True)
        diag_im[i, pl.ds(c, 1), :] += jnp.sum(jnp.where(same, im, 0.0), axis=0, keepdims=True)

    def rest(c, first, count):
        def one(r, carry):
            for i in order:
                measure(i, c, r)
            return carry
        lax.fori_loop(first, first + count, one, 0)

    order = [i for d in (1, 0, 2) for i, point in enumerate(points) if point[0] == d]

    def chunk(c, carry):
        for i in order:
            arrived(i, c)
        rest(c, 0, row_tiles)
        return carry

    lax.fori_loop(0, chunks - 1, chunk, 0)
    last = chunks - 1
    for i in order:
        arrived(i, last)
    rest(last, row_tiles - 1, 1)
    phases = jnp.arctan2(diag_im[...], diag_re[...])
    groups = phases.reshape(3, planes, chunks, cut)
    mean, square = merged([(groups[:, p], jnp.zeros_like(groups[:, p])) for p in range(planes)], 1.0)
    count = float(planes)

    def stat_copy(d, step):
        return pltpu.make_async_remote_copy(
            src_ref=stats.at[d],
            dst_ref=heard[d].at[step - 1],
            send_sem=stat_send[d].at[step - 1],
            recv_sem=stat_recv[d].at[step - 1],
            device_id=beside(d, step),
            device_id_type=MESH,
        )

    for d in range(3):
        stats[d, 0] = mean
        stats[d, 1] = square
        for step in range(1, sizes[d]):
            stat_copy(d, step).start()
        if d == 0 and row_tiles > 1:
            rest(last, 0, row_tiles - 1)
            for i in range(len(points)):
                coherence_ref[i:i + 1, :] = jnp.full((1, LANES), 1.0 / bands, jnp.float32) * jnp.sum(total[i])
        for step in range(1, sizes[d]):
            stat_copy(d, step).wait_recv()
        members = [(mean, square)] + [(heard[d][step - 1, 0], heard[d][step - 1, 1]) for step in range(1, sizes[d])]
        ordered = []
        for slot in range(sizes[d]):
            entry = None
            for step in range(sizes[d]):
                owner = lax.rem(place[d] - step + sizes[d], sizes[d])
                if entry is None:
                    entry = members[step]
                else:
                    entry = tuple(jnp.where(owner == slot, new, old) for new, old in zip(members[step], entry))
            ordered.append(entry)
        mean, square = merged(ordered, count)
        count *= sizes[d]

    lengths = (planes * sizes[0], sizes[1], sizes[2])
    for d in range(3):
        scale = lengths[d] / (2.0 * jnp.pi)
        for c in range(chunks):
            lanes = slice(c * cut, (c + 1) * cut)
            centre_ref[d:d + 1, lanes] = -scale * mean[d, c:c + 1, :]
            spread_ref[d:d + 1, lanes] = scale * scale * (square[d, c:c + 1, :] / count)

    for d in range(3):
        for step in range(1, sizes[d]):
            stat_copy(d, step).wait_send()

    def sent(c, carry):
        for i in range(len(points)):
            if not inner(i):
                copy_of(i, c).wait_send()
        return carry

    lax.fori_loop(0, chunks, sent, 0)


def solution(mesh):
    sizes = tuple(mesh.shape[axis] for axis in AXES)

    def shards(coefficients, shift_blocks):
        planes, bands, width = coefficients.shape[1], coefficients.shape[4], coefficients.shape[5]
        own_planes = coefficients.reshape(2, planes, bands, width)
        chunks = bands // LANES
        pairs = 3 * planes
        vmem = pl.BlockSpec(memory_space=pltpu.VMEM)
        centre, spread, coherence = pl.pallas_call(
            functools.partial(kernel, sizes),
            out_shape=(
                jax.ShapeDtypeStruct((3, bands), jnp.float32),
                jax.ShapeDtypeStruct((3, bands), jnp.float32),
                jax.ShapeDtypeStruct((pairs, LANES), jnp.float32),
            ),
            in_specs=[pl.BlockSpec(memory_space=pltpu.SMEM), pl.BlockSpec(memory_space=pl.ANY)],
            out_specs=(vmem, vmem, vmem),
            scratch_shapes=[
                pltpu.VMEM((2, planes, bands, width), jnp.bfloat16),
                pltpu.VMEM((pairs, chunks, 2, LANES, width), jnp.bfloat16),
                pltpu.VMEM((pairs, 2, bands, width), jnp.bfloat16),
                pltpu.VMEM((pairs, chunks, LANES), jnp.float32),
                pltpu.VMEM((pairs, chunks, LANES), jnp.float32),
                pltpu.VMEM((pairs, 8, LANES), jnp.float32),
                pltpu.VMEM((3, 2, 3, chunks, LANES), jnp.float32),
                [pltpu.VMEM((size - 1, 2, 3, chunks, LANES), jnp.float32) for size in sizes],
                pltpu.SemaphoreType.DMA,
                pltpu.SemaphoreType.DMA((pairs, chunks)),
                pltpu.SemaphoreType.DMA((pairs, chunks)),
                [pltpu.SemaphoreType.DMA((size - 1,)) for size in sizes],
                [pltpu.SemaphoreType.DMA((size - 1,)) for size in sizes],
            ],
            compiler_params=pltpu.CompilerParams(
                collective_id=0, has_side_effects=True, vmem_limit_bytes=60 * 1024 * 1024
            ),
        )(shift_blocks, own_planes)
        return centre, spread, coherence[:, :1].reshape(3, planes, 1, 1)

    in_specs = (P(None, "kx", "ky", "kz", None, None), P())
    out_specs = (P(), P(), P(None, "kx", "ky", "kz"))
    return jax.shard_map(shards, mesh=mesh, in_specs=in_specs, out_specs=out_specs, check_vma=False)
```
